32 devices in a mesh: member: 16 (over z, y, core), slab: 2 (over x).
Axes of the slice: x: 2, y: 2, z: 4, core: 2. Of those that a mesh axis runs over, the one named last changes fastest.
Arguments:
- checkpoint: float32 [16, 2, 4, 256, 256], P('member', None, 'slab'), may hold values from 0 to 1
- adjoint_late: float32 [16, 2, 4, 256, 256], P('member', None, 'slab'), may hold values from -6 to 6
- rate_params: float32 [64, 64], replicated, may hold values from 0.02 to 0.1
- perturbation: float32 [16, 64, 64], P('member'), may hold values from -0.5 to 0.5
Outputs:
- adjoint_early: float32 [16, 2, 4, 256, 256], P('member', None, 'slab')
- param_grad: float32 [64, 64], replicated
The draws below stay inside these ranges and needn't reach their ends.
All inputs are finite; a program needn't handle non-finite values.
Results may differ from the reference program's by a relative error of at most 0.00002.
Values sent between devices are 32-bit elements; how exact they have to be, the bound alone decides.
No kernel may reach another device: no remote copies, remote signals or barrier semaphores. Data moves between devices by JAX's collectives and lax.ppermute only.
A program may use at most 64 MiB of HBM per device.

```python
import math
import jax
import jax.numpy as jnp
from jax import lax

PX = 64
PY = 64
SX = 4
SY = 4
MEMBERS = 16
NX = 256
NY = 256
NZ = 4


def levels(own_key, extent, shards, least, top_value):
    def one(axis_at, shards_of):
        draws = jax.random.uniform(jax.random.fold_in(jax.random.fold_in(own_key, 6), axis_at), (shards_of,), jnp.float32, least / len(shards), top_value / len(shards))
        return jnp.repeat(jnp.exp(draws), extent[axis_at] // shards_of).reshape((-1,) + (1,) * (len(extent) - axis_at - 1))

    loudness = one(*shards[0])
    for cut in shards[1:]:
        loudness = loudness * one(*cut)
    return loudness


def normal_values(stream_key, dims, width, bound, split=(), dtype=jnp.bfloat16):
    loudness = levels(stream_key, dims, split, -0.22, 0.18) if split else 1.0
    entries = jax.random.normal(stream_key, dims, jnp.float32) * width * loudness
    return jnp.minimum(jnp.maximum(entries, -bound), bound).astype(dtype)


def setup_inputs(seed: int = 0) -> dict:
    streams_of = jax.random.split(jax.random.key(seed), 5)
    checkpoint = jnp.clip(1.0 * jax.random.uniform(streams_of[0], (MEMBERS, 2, NZ, NX, NY), jnp.float32) ** levels(streams_of[0], (MEMBERS, 2, NZ, NX, NY), ((0, 16), (2, 2)), -0.2, 0.2), 0.0, 1.0)
    adjoint_late = normal_values(streams_of[1], (MEMBERS, 2, NZ, NX, NY), 1.0, 6.0, ((0, 16), (2, 2)), jnp.float32)
    rate_params = jnp.clip(jnp.exp(jax.random.uniform(streams_of[2], (PX, PY), jnp.float32, math.log(0.02), math.log(0.1))), 0.02, 0.1)
    perturbation = jnp.clip(jax.random.uniform(streams_of[3], (MEMBERS, PX, PY), jnp.float32, -0.5, 0.5) * levels(streams_of[3], (MEMBERS, PX, PY), ((0, 16),), -0.4, 0.0), -0.5, 0.5)
    return {"checkpoint": checkpoint, "adjoint_late": adjoint_late, "rate_params": rate_params, "perturbation": perturbation}


feed_rate = 0.035
substrate_diffusion = 0.16
activator_diffusion = 0.08


def laplace_rim(extended):
    padded = jnp.pad(extended, ((0, 0), (0, 0), (1, 1), (1, 1)))
    center = padded[:, 1:-1, 1:-1, 1:-1]
    summed = padded[:, 2:, 1:-1, 1:-1] + padded[:, :-2, 1:-1, 1:-1]
    summed = summed + padded[:, 1:-1, 2:, 1:-1] + padded[:, 1:-1, :-2, 1:-1]
    summed = summed + padded[:, 1:-1, 1:-1, 2:] + padded[:, 1:-1, 1:-1, :-2]
    return summed - 6.0 * center


def advance(extended, decay_rate):
    laplace = laplace_rim(extended)
    u_field = extended[0, 1:-1]
    v_field = extended[1, 1:-1]
    reaction = u_field * v_field * v_field
    u_new = u_field + substrate_diffusion * laplace[0] - reaction + feed_rate * (1.0 - u_field)
    v_new = v_field + activator_diffusion * laplace[1] + reaction - (feed_rate + decay_rate) * v_field
    return jnp.stack([u_new, v_new])


def pull_back(status, adjoint_ext, decay_rate):
    laplace = laplace_rim(adjoint_ext)
    adj_u = adjoint_ext[0, 1:-1]
    adj_v = adjoint_ext[1, 1:-1]
    uv_prod = status[0] * status[1]
    v_square = status[1] * status[1]
    new_u = adj_u + substrate_diffusion * laplace[0] - (v_square + feed_rate) * adj_u + v_square * adj_v
    new_v = adj_v + activator_diffusion * laplace[1] - 2.0 * uv_prod * adj_u + (2.0 * uv_prod - feed_rate - decay_rate) * adj_v
    return jnp.stack([new_u, new_v])


def expand_params(table):
    return jnp.broadcast_to(table[:, None, :, None], (PX, SX, PY, SY)).reshape(NX, NY)


def patch_total(field):
    return jnp.sum(field.reshape(PX, SX, PY, SY), axis=(1, 3))


def pad_planes(field):
    return jnp.pad(field, ((0, 0), (1, 1), (0, 0), (0, 0)))


def reference(checkpoint, adjoint_late, rate_params, perturbation):
    def one_member(member_item):
        start_state, adjoint_two, member_shift = member_item
        factor = 1.0 + member_shift
        decay_rate = expand_params(rate_params * factor)
        middle = advance(pad_planes(start_state), decay_rate)
        adjoint_one = pull_back(middle, pad_planes(adjoint_two), decay_rate)
        adjoint_zero = pull_back(start_state, pad_planes(adjoint_one), decay_rate)
        cell_grad = -(jnp.sum(middle[1] * adjoint_two[1], 0) + jnp.sum(start_state[1] * adjoint_one[1], 0))
        return adjoint_zero, patch_total(cell_grad) * factor

    adjoint_early, grads = lax.map(one_member, (checkpoint, adjoint_late, perturbation))
    return adjoint_early, jnp.sum(grads, 0) / MEMBERS
```

```python
import functools

import jax
import jax.numpy as jnp
from jax import lax
from jax.experimental import pallas as pl
from jax.experimental.pallas import tpu as pltpu
from jax.sharding import PartitionSpec as P

feed_rate = 0.035
substrate_diffusion = 0.16
activator_diffusion = 0.08

ROWS = 32
VMEM = pl.BlockSpec(memory_space=pltpu.VMEM)
EXACT = lax.Precision.HIGHEST


def stencil(load, step, rows, total):
    first = pl.multiple_of(step * rows, rows)
    here = load(first, rows)
    above = load(pl.multiple_of(jnp.maximum(first - 8, 0), 8), 8)
    below = load(pl.multiple_of(jnp.minimum(first + rows, total - 8), 8), 8)
    above = jnp.where(step > 0, above, 0.0)
    below = jnp.where(first + rows < total, below, 0.0)
    tall = jnp.concatenate([above, here, below], axis=0)
    up = pltpu.roll(tall, 1, 0)[8 : 8 + rows]
    down = pltpu.roll(tall, rows + 15, 0)[8 : 8 + rows]
    columns = here.shape[1]
    lane = lax.broadcasted_iota(jnp.int32, here.shape, 1)
    left = jnp.where(lane == 0, 0.0, pltpu.roll(here, 1, 1))
    right = jnp.where(lane == columns - 1, 0.0, pltpu.roll(here, columns - 1, 1))
    return here, (up + down) + (left + right)


def plane(ref, *lead):
    return lambda start, size: ref[(*lead, pl.ds(start, size), slice(None))]


def spread_matrix(cells, patches):
    row = lax.broadcasted_iota(jnp.int32, (cells, patches), 0)
    column = lax.broadcasted_iota(jnp.int32, (cells, patches), 1)
    return jnp.where(row // (cells // patches) == column, 1.0, 0.0)


def gather_matrix(patches, cells):
    row = lax.broadcasted_iota(jnp.int32, (patches, cells), 0)
    column = lax.broadcasted_iota(jnp.int32, (patches, cells), 1)
    return jnp.where(column // (cells // patches) == row, 1.0, 0.0)


def exact_dot(a, b):
    return jnp.dot(a, b, precision=EXACT, preferred_element_type=jnp.float32)


def local_kernel(sides, ck, ad, rate, pert, part, decay, grad_cells, far_mid):
    near = 1 - lax.rem(lax.axis_index("slab"), 2)
    slots = (near, 1 - near)
    total, columns = ck.shape[3:]
    table = rate[...] * (1.0 + pert[0])
    decay[...] = exact_dot(
        exact_dot(spread_matrix(total, table.shape[0]), table),
        gather_matrix(table.shape[1], columns),
    )

    def rows(step, carry):
        here = pl.ds(pl.multiple_of(step * ROWS, ROWS), ROWS)
        loss = decay[here, :] + feed_rate
        fields = {}
        for name, ref, index in (("u", ck, 0), ("v", ck, 1), ("a", ad, 0), ("b", ad, 1)):
            for s in range(2):
                fields[name, s] = stencil(plane(ref, 0, index, slots[s]), step, ROWS, total)
        lap = {
            (n, s): ring + fields[n, 1 - s][0] - 6.0 * mid for (n, s), (mid, ring) in fields.items()
        }
        cells = 0.0
        for s in range(2):
            u, v, a, b = (fields[n, s][0] for n in "uvab")
            reaction = u * v * v
            u_new = u + substrate_diffusion * lap["u", s] - reaction + feed_rate * (1.0 - u)
            v_new = v + activator_diffusion * lap["v", s] + reaction - loss * v
            alpha = a + substrate_diffusion * lap["a", s] - feed_rate * a
            beta = b + activator_diffusion * lap["b", s] - loss * b
            gap = b - a
            if s < sides:
                part[s, 0, here, :] = u_new
                part[s, 1, here, :] = v_new
                part[s, 2, here, :] = alpha
                part[s, 3, here, :] = beta
                part[s, 4, here, :] = gap
            else:
                alpha = alpha + v_new * v_new * gap
                beta = beta + 2.0 * (u_new * v_new) * gap
                far_mid[0, here, :] = alpha
                far_mid[1, here, :] = beta
            cells = cells + (v_new * b + v * beta)
        grad_cells[here, :] = cells
        return carry

    lax.fori_loop(0, total // ROWS, rows, 0)


def react_kernel(sides, share, *refs):
    part, grad_cells, rate, pert = refs[:4]
    halo, state, late = refs[4 : 4 + sides], refs[4 + sides : 4 + 2 * sides], refs[4 + 2 * sides : 4 + 3 * sides]
    alpha, beta, grad, cells = refs[4 + 3 * sides :]
    total, columns = grad_cells.shape

    def rows(step, carry):
        here = pl.ds(pl.multiple_of(step * ROWS, ROWS), ROWS)
        sum_cells = grad_cells[here, :]
        for s in range(sides):
            halo_v = halo[s][1, here, :]
            u_mid = part[s, 0, here, :] + substrate_diffusion * halo[s][0, here, :]
            v_mid = part[s, 1, here, :] + activator_diffusion * halo_v
            gap = part[s, 4, here, :]
            extra = 2.0 * (u_mid * v_mid) * gap
            alpha[s, here, :] = part[s, 2, here, :] + v_mid * v_mid * gap
            beta[s, here, :] = part[s, 3, here, :] + extra
            sum_cells = sum_cells + (
                (2.0 * activator_diffusion) * halo_v * late[s][here, :] + state[s][1, here, :] * extra
            )
        cells[here, :] = sum_cells
        return carry

    lax.fori_loop(0, total // ROWS, rows, 0)
    patches = rate.shape
    summed = exact_dot(
        exact_dot(gather_matrix(patches[0], total), cells[...]),
        spread_matrix(columns, patches[1]),
    )
    grad[...] = summed * (1.0 + pert[0]) * (-share)


def last_kernel(sides, ck, decay, near_a, near_b, far_a, far_b, early, *refs):
    near = 1 - lax.rem(lax.axis_index("slab"), 2)
    total = decay.shape[0]
    mids = ((near_a, near_b), (far_a, far_b))
    outs = refs[:2]

    def rows(step, carry):
        here = pl.ds(pl.multiple_of(step * ROWS, ROWS), ROWS)
        loss = decay[here, :] + feed_rate
        found = [[stencil(plane(ref), step, ROWS, total) for ref in pair] for pair in mids]
        for s in range(2):
            slot = near if s == 0 else 1 - near
            (a, ring_a), (b, ring_b) = found[s]
            lap_a = ring_a + found[1 - s][0][0] - 6.0 * a
            lap_b = ring_b + found[1 - s][1][0] - 6.0 * b
            u = ck[0, 0, slot, here, :]
            v = ck[0, 1, slot, here, :]
            gap = b - a
            outs[s][0, here, :] = a + substrate_diffusion * lap_a - feed_rate * a + v * v * gap
            outs[s][1, here, :] = b + activator_diffusion * lap_b - loss * b + 2.0 * (u * v) * gap
        return carry

    lax.fori_loop(0, total // ROWS, rows, 0)
    if sides == 1:
        copy = pltpu.make_async_copy(refs[1], early.at[0, :, 1 - near], refs[2])
        copy.start()
        copy.wait()


def call(body, name, outs, flops, args, scratch=(), spaces=None):
    return pl.pallas_call(
        body,
        name=name,
        out_shape=[jax.ShapeDtypeStruct(shape, jnp.float32) for shape in outs],
        in_specs=[VMEM] * len(args),
        out_specs=spaces or [VMEM] * len(outs),
        scratch_shapes=list(scratch),
        compiler_params=pltpu.CompilerParams(vmem_limit_bytes=16 << 20),
        cost_estimate=pl.CostEstimate(flops=flops, bytes_accessed=1 << 20, transcendentals=0),
    )(*args)


def exchange(near, far, sides):
    count = lax.axis_size("slab")
    swaps = []
    for side, value in zip(range(sides), (near, far)):
        pairs = [(i, i + 1) for i in range(side, count - 1, 2)]
        swaps.append(lax.ppermute(value, "slab", pairs + [(j, i) for i, j in pairs]))
    return swaps


def butterfly(value, axis):
    count = lax.axis_size(axis)
    if count & (count - 1):
        return lax.psum(value, axis)
    bit = 1
    while bit < count:
        value = value + lax.ppermute(value, axis, [(i, i ^ bit) for i in range(count)])
        bit *= 2
    return value


def local(checkpoint, adjoint_late, rate_params, perturbation):
    sides = 1 if lax.axis_size("slab") <= 2 else 2
    near = 1 - lax.rem(lax.axis_index("slab"), 2)
    grid = checkpoint.shape[3:]

    def pick(array, first, size, slot):
        found = lax.dynamic_slice(array, (0, first, slot, 0, 0), (1, size, 1, *grid))
        return found.reshape((size, *grid) if size > 1 else grid)

    slots = [near, 1 - near][:sides]
    uv = [pick(checkpoint, 0, 2, s) for s in slots]
    late_b = [pick(adjoint_late, 1, 1, s) for s in slots]
    late_a = [pick(adjoint_late, 0, 1, s) for s in slots]
    halo_uv = exchange(uv[0], uv[-1], sides)
    halo_b = exchange(late_b[0], late_b[-1], sides)
    halo_a = exchange(late_a[0], late_a[-1], sides)

    part, decay, grad_cells, far_mid = call(
        functools.partial(local_kernel, sides),
        "local_terms",
        [(sides, 5, *grid), grid, grid, (2, *grid)],
        1 << 28,
        (checkpoint, adjoint_late, rate_params, perturbation),
    )

    share = 1.0 / lax.axis_size("member")
    alpha, beta, grad = call(
        functools.partial(react_kernel, sides, share),
        "reaction",
        [(sides, *grid), (sides, *grid), rate_params.shape],
        1 << 26,
        (part, grad_cells, rate_params, perturbation, *halo_uv, *uv, *late_b),
        [pltpu.VMEM(grid, jnp.float32)],
    )

    mid_b = [beta[s] + activator_diffusion * halo_b[s] for s in range(sides)]
    halo_mid_b = exchange(mid_b[0], mid_b[-1], sides)
    mid_a = [alpha[s] + substrate_diffusion * halo_a[s] for s in range(sides)]
    halo_mid_a = exchange(mid_a[0], mid_a[-1], sides)
    if sides == 1:
        mid_a.append(far_mid[0])
        mid_b.append(far_mid[1])

    whole = [(2, *grid)] * sides
    early, *partial = call(
        functools.partial(last_kernel, sides),
        "last_step",
        [checkpoint.shape, *whole],
        1 << 27,
        (checkpoint, decay, mid_a[0], mid_b[0], mid_a[1], mid_b[1]),
        [pltpu.VMEM((2, *grid), jnp.float32), pltpu.SemaphoreType.DMA] if sides == 1 else [],
        [pl.BlockSpec(memory_space=pl.ANY)] + [VMEM] * sides,
    )
    grad = butterfly(butterfly(grad, "member"), "slab")

    for field, rate, halo in (
        (1, activator_diffusion, halo_mid_b),
        (0, substrate_diffusion, halo_mid_a),
    ):
        for s in range(sides):
            plane_out = partial[s][field] + rate * halo[s]
            early = lax.dynamic_update_slice(early, plane_out[None, None, None], (0, field, slots[s], 0, 0))
    return early, grad


def solution(mesh):
    return jax.shard_map(
        local,
        mesh=mesh,
        in_specs=(
            P("member", None, "slab", None, None),
            P("member", None, "slab", None, None),
            P(),
            P("member", None, None),
        ),
        out_specs=(P("member", None, "slab", None, None), P()),
        check_vma=False,
    )
```

```python
import functools

import jax
import jax.numpy as jnp
from jax import lax
from jax.experimental import pallas as pl
from jax.experimental.pallas import tpu as pltpu
from jax.sharding import PartitionSpec as P


feed_rate = 0.035
substrate_diffusion = 0.16
activator_diffusion = 0.08


ROWS = 32
PIECES = 2
VMEM = pl.BlockSpec(memory_space=pltpu.VMEM)
HBM = pl.BlockSpec(memory_space=pl.ANY)
STAY = pl.BlockSpec(memory_space=pltpu.HBM)
EXACT = lax.Precision.HIGHEST


def stencil(load, step, rows, total):
    first = pl.multiple_of(step * rows, rows)
    here = load(first, rows)
    above = load(pl.multiple_of(jnp.maximum(first - 8, 0), 8), 8)
    below = load(pl.multiple_of(jnp.minimum(first + rows, total - 8), 8), 8)
    above = jnp.where(step > 0, above, 0.0)
    below = jnp.where(first + rows < total, below, 0.0)
    tall = jnp.concatenate([above, here, below], axis=0)
    up = pltpu.roll(tall, 1, 0)[8 : 8 + rows]
    down = pltpu.roll(tall, rows + 15, 0)[8 : 8 + rows]
    columns = here.shape[1]
    lane = lax.broadcasted_iota(jnp.int32, here.shape, 1)
    left = jnp.where(lane == 0, 0.0, pltpu.roll(here, 1, 1))
    right = jnp.where(lane == columns - 1, 0.0, pltpu.roll(here, columns - 1, 1))
    return here, (up + down) + (left + right)


def plane(ref, *lead):
    return lambda start, size: ref[(*lead, pl.ds(start, size), slice(None))]


def spread_matrix(cells, patches):
    row = lax.broadcasted_iota(jnp.int32, (cells, patches), 0)
    column = lax.broadcasted_iota(jnp.int32, (cells, patches), 1)
    return jnp.where(row // (cells // patches) == column, 1.0, 0.0)


def gather_matrix(patches, cells):
    row = lax.broadcasted_iota(jnp.int32, (patches, cells), 0)
    column = lax.broadcasted_iota(jnp.int32, (patches, cells), 1)
    return jnp.where(column // (cells // patches) == row, 1.0, 0.0)


def exact_dot(a, b):
    return jnp.dot(a, b, precision=EXACT, preferred_element_type=jnp.float32)


def local_kernel(sides, state, late, rate, pert, part, decay, grad_cells, far_mid, products, ck, ad, sems):
    near = 1 - lax.rem(lax.axis_index("slab"), 2)
    copies = [pltpu.make_async_copy(state, ck, sems.at[0]), pltpu.make_async_copy(late, ad, sems.at[1])]
    for copy in copies:
        copy.start()
    slots = (near, 1 - near)
    total, columns = ck.shape[3:]
    table = rate[...] * (1.0 + pert[0])
    decay[...] = exact_dot(
        exact_dot(spread_matrix(total, table.shape[0]), table),
        gather_matrix(table.shape[1], columns),
    )

    for copy in copies:
        copy.wait()

    def rows(step, carry):
        here = pl.ds(pl.multiple_of(step * ROWS, ROWS), ROWS)
        loss = decay[here, :] + feed_rate
        fields = {}
        for name, ref, index in (("u", ck, 0), ("v", ck, 1), ("a", ad, 0), ("b", ad, 1)):
            for s in range(2):
                fields[name, s] = stencil(plane(ref, 0, index, slots[s]), step, ROWS, total)
        lap = {
            (n, s): ring + fields[n, 1 - s][0] - 6.0 * mid for (n, s), (mid, ring) in fields.items()
        }
        cells = 0.0
        for s in range(2):
            u, v, a, b = (fields[n, s][0] for n in "uvab")
            reaction = u * v * v
            u_new = u + substrate_diffusion * lap["u", s] - reaction + feed_rate * (1.0 - u)
            v_new = v + activator_diffusion * lap["v", s] + reaction - loss * v
            alpha = a + substrate_diffusion * lap["a", s] - feed_rate * a
            beta = b + activator_diffusion * lap["b", s] - loss * b
            gap = b - a
            products[s, 0, here, :] = v * v
            products[s, 1, here, :] = 2.0 * (u * v)
            if s < sides:
                part[s, 0, here, :] = u_new
                part[s, 1, here, :] = v_new
                part[s, 2, here, :] = alpha
                part[s, 3, here, :] = beta
                part[s, 4, here, :] = gap
            else:
                alpha = alpha + v_new * v_new * gap
                beta = beta + 2.0 * (u_new * v_new) * gap
                far_mid[0, here, :] = alpha
                far_mid[1, here, :] = beta
            cells = cells + (v_new * b + v * beta)
        grad_cells[here, :] = cells
        return carry

    lax.fori_loop(0, total // ROWS, rows, 0)


def react_kernel(sides, share, *refs):
    part, grad_cells, rate, pert = refs[:4]
    halo_u, halo_v, state_v, late_b = (refs[4 + i * sides : 4 + (i + 1) * sides] for i in range(4))
    alpha, beta, grad, cells = refs[4 + 4 * sides :]
    total, columns = grad_cells.shape

    def rows(step, carry):
        here = pl.ds(pl.multiple_of(step * ROWS, ROWS), ROWS)
        sum_cells = grad_cells[here, :]
        for s in range(sides):
            v_in = halo_v[s][here, :]
            u_mid = part[s, 0, here, :] + substrate_diffusion * halo_u[s][here, :]
            v_mid = part[s, 1, here, :] + activator_diffusion * v_in
            gap = part[s, 4, here, :]
            extra = 2.0 * (u_mid * v_mid) * gap
            alpha[s, here, :] = part[s, 2, here, :] + v_mid * v_mid * gap
            beta[s, here, :] = part[s, 3, here, :] + extra
            sum_cells = sum_cells + (
                (2.0 * activator_diffusion) * v_in * late_b[s][here, :] + state_v[s][here, :] * extra
            )
        cells[here, :] = sum_cells
        return carry

    lax.fori_loop(0, total // ROWS, rows, 0)
    patches = rate.shape
    summed = exact_dot(
        exact_dot(gather_matrix(patches[0], total), cells[...]),
        spread_matrix(columns, patches[1]),
    )
    summed = summed * (1.0 + pert[0]) * (-share)
    tall = grad.shape[0]
    grad[...] = jnp.concatenate(
        [summed[first : first + tall] for first in range(0, patches[0], tall)], axis=1
    )


def last_kernel(sides, products, decay, alpha, beta, *refs):
    near = 1 - lax.rem(lax.axis_index("slab"), 2)
    total = decay.shape[0]

    def middle(base, halo, slot, rate):
        def load(start, size):
            here = pl.ds(start, size)
            return base[slot, here, :] + rate * halo[here, :]

        return load

    mids = [
        (
            middle(alpha, refs[s], s, substrate_diffusion),
            middle(beta, refs[sides + s], s, activator_diffusion),
        )
        for s in range(sides)
    ]
    refs = refs[2 * sides :]
    if sides == 1:
        far_mid, *refs = refs
        mids.append((plane(far_mid, 0), plane(far_mid, 1)))
    early, *outs = refs

    def rows(step, carry):
        here = pl.ds(pl.multiple_of(step * ROWS, ROWS), ROWS)
        loss = decay[here, :] + feed_rate
        found = [[stencil(load, step, ROWS, total) for load in pair] for pair in mids]
        for s in range(2):
            (a, ring_a), (b, ring_b) = found[s]
            lap_a = ring_a + found[1 - s][0][0] - 6.0 * a
            lap_b = ring_b + found[1 - s][1][0] - 6.0 * b
            gap = b - a
            outs[s][0, here, :] = (
                a + substrate_diffusion * lap_a - feed_rate * a + products[s, 0, here, :] * gap
            )
            outs[s][1, here, :] = (
                b + activator_diffusion * lap_b - loss * b + products[s, 1, here, :] * gap
            )
        return carry

    lax.fori_loop(0, total // ROWS, rows, 0)
    if sides == 1:
        copy = pltpu.make_async_copy(outs[1], early.at[0, :, 1 - near], outs[2])
        copy.start()
        copy.wait()


def finish_kernel(sides, before, grad, arrived, *refs):
    near = 1 - lax.rem(lax.axis_index("slab"), 2)
    partial, halo = refs[:sides], refs[sides : 2 * sides]
    early, total, planes, table, sems = refs[2 * sides :]
    copies = []

    def send(source, target):
        copies.append(pltpu.make_async_copy(source, target, sems.at[len(copies)]))
        copies[-1].start()

    rows = planes.shape[1]
    for s in range(sides):
        slot = near if s == 0 else 1 - near
        for first in range(0, rows, rows // PIECES):
            here = pl.ds(first, rows // PIECES)
            planes[s, here, :] = partial[s][0, here, :] + substrate_diffusion * halo[s][here, :]
            send(planes.at[s, here], early.at[0, 0, slot, here])
    tall, columns = grad.shape[0], total.shape[1]
    for fold in range(grad.shape[1] // columns):
        part = slice(fold * columns, (fold + 1) * columns)
        table[fold * tall : (fold + 1) * tall, :] = grad[:, part] + arrived[:, part]
    send(table, total)
    for copy in copies:
        copy.wait()


def call(body, outs, flops, args, scratch=(), writes=None, reads=None, aliases={}):
    return pl.pallas_call(
        body,
        out_shape=[jax.ShapeDtypeStruct(shape, jnp.float32) for shape in outs],
        in_specs=reads or [VMEM] * len(args),
        out_specs=writes or [VMEM] * len(outs),
        input_output_aliases=aliases,
        scratch_shapes=list(scratch),
        compiler_params=pltpu.CompilerParams(vmem_limit_bytes=16 << 20),
        cost_estimate=pl.CostEstimate(flops=flops, bytes_accessed=1 << 20, transcendentals=0),
    )(*args)


def exchange(near, far, sides):
    count = lax.axis_size("slab")
    swaps = []
    for side, value in zip(range(sides), (near, far)):
        pairs = [(i, i + 1) for i in range(side, count - 1, 2)]
        swaps.append(lax.ppermute(value, "slab", pairs + [(j, i) for i, j in pairs]))
    return swaps


def total_of(value):
    last = jnp.zeros_like(value)
    hops = []
    for axis in ("member", "slab"):
        count = lax.axis_size(axis)
        if count & (count - 1):
            value = lax.psum(value, axis)
        else:
            hops += [(axis, count, 1 << bit) for bit in range(count.bit_length() - 1)]
    for index, (axis, count, bit) in enumerate(hops):
        last = lax.ppermute(value, axis, [(i, i ^ bit) for i in range(count)])
        if index + 1 < len(hops):
            value = value + last
    return value, last


def folded(shape):
    fold = max(128 // shape[1], 1)
    return (shape[0] // fold, shape[1] * fold) if shape[0] % (8 * fold) == 0 else shape


def local(checkpoint, adjoint_late, rate_params, perturbation):
    sides = 1 if lax.axis_size("slab") <= 2 else 2
    near = 1 - lax.rem(lax.axis_index("slab"), 2)
    grid = checkpoint.shape[3:]

    def pick(array, field, slot):
        return lax.dynamic_slice(array, (0, field, slot, 0, 0), (1, 1, 1, *grid)).reshape(grid)

    slots = [near, 1 - near][:sides]
    u = [pick(checkpoint, 0, s) for s in slots]
    halo_u = exchange(u[0], u[-1], sides)
    slots, _ = lax.optimization_barrier((slots, u))
    v = [pick(checkpoint, 1, s) for s in slots]
    halo_v = exchange(v[0], v[-1], sides)
    late_b = [pick(adjoint_late, 1, s) for s in slots]
    late_a = [pick(adjoint_late, 0, s) for s in slots]
    halo_b = exchange(late_b[0], late_b[-1], sides)
    halo_a = exchange(late_a[0], late_a[-1], sides)

    part, decay, grad_cells, far_mid, products = call(
        functools.partial(local_kernel, sides),
        [(sides, 5, *grid), grid, grid, (2, *grid), (2, 2, *grid)],
        1 << 28,
        (checkpoint, adjoint_late, rate_params, perturbation),
        [
            pltpu.VMEM(checkpoint.shape, jnp.float32),
            pltpu.VMEM(adjoint_late.shape, jnp.float32),
            pltpu.SemaphoreType.DMA((2,)),
        ],
        reads=[STAY, STAY, VMEM, VMEM],
    )

    share = 1.0 / lax.axis_size("member")
    alpha, beta, grad = call(
        functools.partial(react_kernel, sides, share),
        [(sides, *grid), (sides, *grid), folded(rate_params.shape)],
        1 << 26,
        (part, grad_cells, rate_params, perturbation, *halo_u, *halo_v, *v, *late_b),
        [pltpu.VMEM(grid, jnp.float32)],
    )

    mid_b = [beta[s] + activator_diffusion * halo_b[s] for s in range(sides)]
    halo_mid_b = exchange(mid_b[0], mid_b[-1], sides)
    mid_a = [alpha[s] + substrate_diffusion * halo_a[s] for s in range(sides)]
    halo_mid_a = exchange(mid_a[0], mid_a[-1], sides)

    early, *partial = call(
        functools.partial(last_kernel, sides),
        [checkpoint.shape] + [(2, *grid)] * sides,
        1 << 27,
        (products, decay, alpha, beta, *halo_a, *halo_b, *([far_mid] if sides == 1 else [])),
        [pltpu.VMEM((2, *grid), jnp.float32), pltpu.SemaphoreType.DMA] if sides == 1 else [],
        [HBM] + [VMEM] * sides,
    )
    for s in range(sides):
        done = partial[s][1] + activator_diffusion * halo_mid_b[s]
        early = lax.dynamic_update_slice(early, done[None, None, None], (0, 1, slots[s], 0, 0))
    return call(
        functools.partial(finish_kernel, sides),
        [checkpoint.shape, rate_params.shape],
        1 << 22,
        (early, *total_of(grad), *partial, *halo_mid_a),
        [
            pltpu.VMEM((sides, *grid), jnp.float32),
            pltpu.VMEM(rate_params.shape, jnp.float32),
            pltpu.SemaphoreType.DMA((PIECES * sides + 1,)),
        ],
        [HBM, HBM],
        [HBM] + [VMEM] * (2 + 2 * sides),
        {0: 0},
    )


def solution(mesh):
    return jax.shard_map(
        local,
        mesh=mesh,
        in_specs=(
            P("member", None, "slab", None, None),
            P("member", None, "slab", None, None),
            P(),
            P("member", None, None),
        ),
        out_specs=(P("member", None, "slab", None, None), P()),
        check_vma=False,
    )
```
